32 devices in a mesh: space: 16 (over z, y, x), grp: 2 (over core).
Axes of the slice: x: 2, y: 2, z: 4, core: 2. Of those that a mesh axis runs over, the one named last changes fastest.
Arguments:
- echoes: bfloat16 [160, 300, 2048], P(('space', 'grp'))
- frame_count: int32 [160], replicated, may hold values from 0 to 300, as said below
- clutter_rank: int32 [160], replicated, may hold values from 1 to 24
- noise_rank: int32 [160], replicated, may hold values from 48 to 96
- start_basis: float32 [300, 96], replicated, may hold values from -6 to 6
Outputs:
- volume: float32 [300, 163840], P(None, ('space', 'grp'))
- power: float32 [163840], P(('space', 'grp'))
The draws below stay inside these ranges and needn't reach their ends.
Inputs may be any that keep to these rules, and one draw needn't show every extreme that they name: `frame_count`: within each holder's 5 consecutive slots the slots with frames come first and the others have 0 frames; every holder has 1 to 5 slots with frames, some holder has all 5; two holders with the same grp index whose space indices lie half the space axis apart have at most 6 slots with frames together; a slot with frames has 150 or more.
All inputs are finite; a program needn't handle non-finite values.
Results may differ from the reference program's by a relative error of at most 0.0056.
Values may be sent and summed in bfloat16 or wider, within the bound.
No kernel may reach another device: no remote copies, remote signals or barrier semaphores. Data moves between devices by JAX's collectives and lax.ppermute only.
A program may use at most 128 MiB of HBM per device.

```python
import jax
import jax.numpy as jnp
from jax import lax

F = 300
V = 2048
K = 96
ITERS = 4
HOLD = 5
OWN = 3
BLOCKS = 160
N_SPACE = 16
N_GRP = 2


def live_counts(key):
    half_space = N_SPACE // 2
    first_key, second_key, third_key = jax.random.split(jax.random.fold_in(key, 7), 3)
    totals = jax.random.randint(first_key, (half_space, N_GRP), OWN + 2, 2 * OWN + 1)
    rows = jnp.arange(half_space)[:, None]
    cols = jnp.arange(N_GRP)[None, :]
    corner = (rows == 0) & (cols == 0)
    last_pair = (rows == half_space - 1) & (cols == N_GRP - 1)
    totals = jnp.where(corner, 2 * OWN, totals)
    lowest = OWN + 1
    highest = jnp.minimum(HOLD, totals - 1)
    random_bits = jax.random.randint(second_key, (half_space, N_GRP), 0, 1 << 20)
    larger = lowest + random_bits % (highest - lowest + 1)
    larger = jnp.where(corner, HOLD, larger)
    smaller = totals - larger
    flip_bits = jax.random.randint(third_key, (half_space, N_GRP), 0, 2)
    flip_bits = jnp.where(corner | last_pair, 0, flip_bits)
    first_counts = jnp.where(flip_bits == 0, larger, smaller)
    second_counts = jnp.where(flip_bits == 0, smaller, larger)
    return jnp.concatenate([first_counts, second_counts], axis=0).reshape(-1)


def draw_frame_count(key, part):
    counts = live_counts(key)
    slots = jnp.arange(HOLD)
    live = slots[None, :] < counts[:, None]
    frames = jax.random.randint(jax.random.fold_in(key, 11), (N_SPACE * N_GRP, HOLD), F // 2, F + 1)
    return jnp.where(live, frames, 0).reshape(BLOCKS).astype(jnp.int32)


def draw_echoes(key, part):
    value_key = jax.random.fold_in(jax.random.fold_in(key, 3), 0)
    position = jnp.arange(BLOCKS, dtype=jnp.float32) / max(BLOCKS - 1, 1)
    scales = 3.0 ** position
    values = jnp.clip(jax.random.normal(value_key, (BLOCKS, F, V), jnp.float32), -6.0, 6.0)
    return (values * scales[:, None, None]).astype(jnp.bfloat16)


def with_ends(array, rng, low, high):
    shape = array.shape
    place = [jax.random.randint(jax.random.fold_in(rng, axis), (), 0, shape[axis]) for axis in range(len(shape))]
    array = array.at[tuple(place)].set(low)
    longest = shape.index(max(shape))
    place[longest] = (place[longest] + 1) % shape[longest]
    return array.at[tuple(place)].set(high)


def bell_draw(stream_key, dims, scale, limit, kind=jnp.bfloat16):
    result = scale * jax.random.normal(stream_key, dims, jnp.float32)
    return jnp.clip(result, min=-limit, max=limit).astype(kind)


def setup_inputs(seed: int = 0) -> dict:
    arg_keys = jax.random.split(jax.random.key(seed), 6)
    echoes = draw_echoes(jax.random.fold_in(arg_keys[5], 71), 0)
    frame_count = draw_frame_count(jax.random.fold_in(arg_keys[5], 71), 0)
    clutter_rank = with_ends(jax.random.randint(arg_keys[2], (BLOCKS,), 1, K // 4 + 1), jax.random.fold_in(arg_keys[2], 1), 1, (K // 4 + 1) - 1).astype(jnp.int32)
    noise_rank = with_ends(jax.random.randint(arg_keys[3], (BLOCKS,), K // 2, K + 1), jax.random.fold_in(arg_keys[3], 1), K // 2, K).astype(jnp.int32)
    start_basis = bell_draw(arg_keys[4], (F, K), 1.0, 6.0, jnp.float32)
    return {"echoes": echoes, "frame_count": frame_count, "clutter_rank": clutter_rank, "noise_rank": noise_rank, "start_basis": start_basis}


def filter_block(echo_block, frame_total, clutter_cut, noise_cut, initial):
    frames = jnp.arange(echo_block.shape[0], dtype=jnp.int32)
    frame_mask = (frames < frame_total).astype(jnp.bfloat16)
    padding_diag = (frames >= frame_total).astype(jnp.float32)
    masked = echo_block * frame_mask[:, None]
    gram_matrix = jnp.dot(masked.astype(jnp.float32), masked.T.astype(jnp.float32), preferred_element_type=jnp.float32) + jnp.diag(padding_diag)
    subspace = initial
    for iteration in range(ITERS):
        product = jnp.dot(gram_matrix, subspace, precision=lax.Precision.HIGHEST)
        inner_gram = jnp.dot(product.T, product, precision=lax.Precision.HIGHEST)
        factor = jnp.linalg.cholesky(inner_gram)
        subspace = jax.scipy.linalg.solve_triangular(factor, product.T, lower=True).T
    basis = subspace.astype(jnp.bfloat16)
    coefficients = jnp.dot(basis.T.astype(jnp.float32), masked.astype(jnp.float32), preferred_element_type=jnp.float32)
    columns = jnp.arange(basis.shape[1], dtype=jnp.int32)
    band_mask = ((columns >= clutter_cut) & (columns < noise_cut)).astype(jnp.float32)
    coefficients = (coefficients * band_mask[:, None]).astype(jnp.bfloat16)
    return jnp.dot(basis.astype(jnp.float32), coefficients.astype(jnp.float32), preferred_element_type=jnp.float32).astype(jnp.bfloat16)

def reference(echoes, frame_count, clutter_rank, noise_rank, start_basis):

    def one_block(block_items):
        return filter_block(block_items[0], block_items[1], block_items[2], block_items[3], start_basis)
    cleaned = lax.map(one_block, (echoes, frame_count, clutter_rank, noise_rank))
    width = cleaned.shape[2]
    half_width = width // 2
    window = jnp.sin(jnp.pi * (jnp.arange(width, dtype=jnp.float32) + 0.5) / width) ** 2
    upper_half = cleaned[:, :, half_width:].astype(jnp.float32) * window[half_width:]
    lower_half = cleaned[:, :, :half_width].astype(jnp.float32) * window[:half_width]
    following = jnp.concatenate([lower_half[1:], jnp.zeros_like(lower_half[:1])], axis=0)
    regions = upper_half + following
    frames_total = regions.shape[1]
    volume = jnp.transpose(regions, (1, 0, 2)).reshape(frames_total, -1)
    strength = jnp.sum(volume * volume, axis=0) / frames_total
    power = strength / (jnp.mean(strength) + 1e-06)
    return (volume, power)
```

```python
import functools

import jax
import jax.numpy as jnp
from jax import lax
from jax.experimental import pallas as pl
from jax.experimental.pallas import tpu as pltpu
from jax.sharding import PartitionSpec as P

ITERS = 4
LANES = 128
SLOTS = 8
PANEL = 8
SUPER = 32
HIGHEST = lax.Precision.HIGHEST


def round_up(value, unit):
    return -(-value // unit) * unit


def device_index():
    return lax.axis_index("space") * lax.axis_size("grp") + lax.axis_index("grp")


def inverse_factors(rows_ref, scaled_ref, out_ref, order, hold, out_stride):
    lane = lax.broadcasted_iota(jnp.int32, (SLOTS, LANES), 1)

    def spread(value, index):
        return jnp.broadcast_to(value[:, index : index + 1], (SLOTS, LANES))

    for start in range(0, order, SUPER):
        stop = min(start + SUPER, order)
        for base in range(start, stop, PANEL):
            panel = (lane >= base) & (lane < base + PANEL)
            rows = [rows_ref[(base + r) * SLOTS : (base + r + 1) * SLOTS, :] for r in range(PANEL)]
            block = {
                (r, c): spread(rows[r], base + c) for r in range(PANEL) for c in range(r, PANEL)
            }
            rows = [
                jnp.where(panel, jnp.where(lane == base + r, 1.0, 0.0), rows[r])
                for r in range(PANEL)
            ]
            scaled = []
            for j in range(PANEL):
                inverse = 1.0 / block[j, j]
                scaled.append(rows[j] * inverse)
                for r in range(j + 1, PANEL):
                    factor = block[j, r] * inverse
                    rows[r] = rows[r] - factor * rows[j]
                    for c in range(r, PANEL):
                        block[r, c] = block[r, c] - factor * block[j, c]
            for j in range(PANEL):
                out_ref[pl.ds(base + j, SLOTS, stride=out_stride), :] = jnp.where(
                    lane < base + PANEL, rows[j] * lax.rsqrt(block[j, j]), 0.0
                )
            if stop < order:
                later = (lane >= base + PANEL) & (lane < stop)
                for j in range(PANEL):
                    rows_ref[(base + j) * SLOTS : (base + j + 1) * SLOTS, :] = jnp.where(
                        later, 0.0, rows[j]
                    )
                    at = base - start + j
                    scaled_ref[at * SLOTS : (at + 1) * SLOTS, :] = scaled[j]
            for r in range(base + PANEL, stop):
                total = jnp.where(panel, 0.0, rows_ref[r * SLOTS : (r + 1) * SLOTS, :])
                for j in range(PANEL):
                    total = total - spread(scaled[j], r) * rows[j]
                rows_ref[r * SLOTS : (r + 1) * SLOTS, :] = total
        if stop < order:
            rest = order - stop
            wide_lane = lax.broadcasted_iota(jnp.int32, (rest, LANES), 1)
            done = (wide_lane >= start) & (wide_lane < stop)
            for b in range(hold):
                upper = rows_ref[pl.ds(start * SLOTS + b, stop - start, stride=SLOTS), :]
                lower = scaled_ref[pl.ds(b, stop - start, stride=SLOTS), :]
                update = jnp.dot(
                    lower.T[stop:order, :],
                    upper,
                    precision=HIGHEST,
                    preferred_element_type=jnp.float32,
                )
                where = pl.ds(stop * SLOTS + b, rest, stride=SLOTS)
                rows_ref[where, :] = jnp.where(done, 0.0, rows_ref[where, :]) - update


def basis_kernel(
    frame_ref,
    clutter_ref,
    noise_ref,
    start_ref,
    echo_hbm,
    basis_ref,
    border_ref,
    echo_ref,
    sems,
    gram_ref,
    sub_ref,
    prod_ref,
    rows_ref,
    scaled_ref,
    factor_ref,
):
    hold, frames, width = echo_hbm.shape
    order = start_ref.shape[1]
    tall = basis_ref.shape[1]
    deep = sub_ref.shape[1]
    half = width // 2
    first = device_index() * hold
    copies = [
        pltpu.make_async_copy(echo_hbm.at[b], echo_ref.at[b], sems.at[b]) for b in range(hold)
    ]
    for copy in copies:
        copy.start()
    sub_ref[...] = jnp.zeros_like(sub_ref)
    prod_ref[...] = jnp.zeros_like(prod_ref)
    rows_ref[...] = jnp.zeros_like(rows_ref)
    factor_ref[...] = jnp.zeros_like(factor_ref)
    gram_ref[...] = jnp.zeros_like(gram_ref)
    for b in range(hold):
        sub_ref[b, :frames, :order] = start_ref[...]
    row_at = lax.broadcasted_iota(jnp.int32, (frames, frames), 0)
    column_at = lax.broadcasted_iota(jnp.int32, (frames, frames), 1)
    for b in range(hold):
        copies[b].wait()
        echo = echo_ref[b]
        valid = frame_ref[first + b]
        gram = lax.dot_general(
            echo, echo, (((1,), (1,)), ((), ())), preferred_element_type=jnp.float32
        )
        padding = jnp.where((row_at == column_at) & (row_at >= valid), 1.0, 0.0)
        gram_ref[b, :frames, :frames] = jnp.where(
            (row_at < valid) & (column_at < valid), gram, padding
        )

    def iteration(_, carry):
        for b in range(hold):
            product = jnp.dot(
                gram_ref[b], sub_ref[b], precision=HIGHEST, preferred_element_type=jnp.float32
            )
            prod_ref[b, :tall, :] = product
            whole = prod_ref[b]
            inner = lax.dot_general(
                whole,
                whole,
                (((0,), (0,)), ((), ())),
                precision=HIGHEST,
                preferred_element_type=jnp.float32,
            )
            rows_ref[pl.ds(b, order, stride=SLOTS), :] = inner[:order, :]
        inverse_factors(rows_ref, scaled_ref, factor_ref, order, hold, LANES)
        for b in range(hold):
            sub_ref[b, :tall, :] = lax.dot_general(
                prod_ref[b, :tall, :],
                factor_ref[b * LANES : (b + 1) * LANES, :],
                (((1,), (1,)), ((), ())),
                precision=HIGHEST,
                preferred_element_type=jnp.float32,
            )
        return carry

    lax.fori_loop(0, ITERS, iteration, 0)
    for b in range(hold):
        basis_ref[b] = sub_ref[b, :tall, :].astype(jnp.bfloat16)
    basis = sub_ref[0].T.astype(jnp.bfloat16)[:order, :]
    frame_at = lax.broadcasted_iota(jnp.int32, (order, frames), 1)
    kept = jnp.where(frame_at < frame_ref[first], basis[:, :frames], jnp.zeros((), jnp.bfloat16))
    low = jnp.dot(kept, echo_ref[0, :, :half], preferred_element_type=jnp.float32)
    column = lax.broadcasted_iota(jnp.int32, (order, 1), 0)
    band = (column >= clutter_ref[first]) & (column < noise_ref[first])
    border_ref[:, :half] = jnp.where(band, low, 0.0).astype(jnp.bfloat16)
    border_ref[:, half:] = basis


def find_bases(echoes, frame_count, clutter_rank, noise_rank, start_basis):
    hold, frames, width = echoes.shape
    order = start_basis.shape[1]
    tall = round_up(frames, 16)
    deep = round_up(frames, LANES)
    smem = pl.BlockSpec(memory_space=pltpu.SMEM)
    vmem = pl.BlockSpec(memory_space=pltpu.VMEM)
    return pl.pallas_call(
        basis_kernel,
        out_shape=(
            jax.ShapeDtypeStruct((hold, tall, LANES), jnp.bfloat16),
            jax.ShapeDtypeStruct((order, width // 2 + deep), jnp.bfloat16),
        ),
        in_specs=[smem, smem, smem, vmem, pl.BlockSpec(memory_space=pl.ANY)],
        out_specs=(vmem, vmem),
        scratch_shapes=[
            pltpu.VMEM((hold, frames, width), jnp.bfloat16),
            pltpu.SemaphoreType.DMA((hold,)),
            pltpu.VMEM((hold, tall, deep), jnp.float32),
            pltpu.VMEM((hold, deep, LANES), jnp.float32),
            pltpu.VMEM((hold, deep, LANES), jnp.float32),
            pltpu.VMEM((order * SLOTS, LANES), jnp.float32),
            pltpu.VMEM((SUPER * SLOTS, LANES), jnp.float32),
            pltpu.VMEM((SLOTS * LANES, LANES), jnp.float32),
        ],
        name="find_bases",
    )(frame_count, clutter_rank, noise_rank, start_basis, echoes)


def projected(basis, echo, valid, low, high, order):
    frames = echo.shape[0]
    frame_at = lax.broadcasted_iota(jnp.int32, (order, frames), 1)
    flipped = basis.astype(jnp.float32).T.astype(jnp.bfloat16)[:order, :frames]
    kept = jnp.where(frame_at < valid, flipped, jnp.zeros((), jnp.bfloat16))
    coefficients = jnp.dot(kept, echo, preferred_element_type=jnp.float32)
    column = lax.broadcasted_iota(jnp.int32, (order, 1), 0)
    band = (column >= low) & (column < high)
    coefficients = jnp.where(band, coefficients, 0.0).astype(jnp.bfloat16)
    cleaned = jnp.dot(basis[:frames, :order], coefficients, preferred_element_type=jnp.float32)
    return cleaned.astype(jnp.bfloat16).astype(jnp.float32)


def region_kernel(
    frame_ref,
    clutter_ref,
    noise_ref,
    window_ref,
    upper_ref,
    lower_ref,
    basis_ref,
    volume_ref,
    strength_ref,
    order,
):
    hold = basis_ref.shape[0]
    frames, half = volume_ref.shape
    region = pl.program_id(0)
    at = device_index() * hold + region
    own = projected(
        basis_ref[region, :, :], upper_ref[0], frame_ref[at], clutter_ref[at], noise_ref[at], order
    )
    total = own * window_ref[:, half:]
    volume_ref[...] = total

    @pl.when(region < hold - 1)
    def _():
        next_one = projected(
            basis_ref[region + 1, :, :],
            lower_ref[0],
            frame_ref[at + 1],
            clutter_ref[at + 1],
            noise_ref[at + 1],
            order,
        )
        both = volume_ref[...] + next_one * window_ref[:, :half]
        volume_ref[...] = both
        strength_ref[...] = jnp.sum(both * both, axis=0, keepdims=True) / frames


def compound(echoes, basis, window, frame_count, clutter_rank, noise_rank, order):
    hold, frames, width = echoes.shape
    half = width // 2
    smem = pl.BlockSpec(memory_space=pltpu.SMEM)
    return pl.pallas_call(
        functools.partial(region_kernel, order=order),
        grid=(hold,),
        out_shape=(
            jax.ShapeDtypeStruct((frames, hold * half), jnp.float32),
            jax.ShapeDtypeStruct((1, hold * half), jnp.float32),
        ),
        in_specs=[
            smem,
            smem,
            smem,
            pl.BlockSpec((1, width), lambda r: (0, 0)),
            pl.BlockSpec((1, frames, half), lambda r: (r, 0, 1)),
            pl.BlockSpec((1, frames, half), lambda r: (jnp.minimum(r + 1, hold - 1), 0, 0)),
            pl.BlockSpec(basis.shape, lambda r: (0, 0, 0)),
        ],
        out_specs=(
            pl.BlockSpec((frames, half), lambda r: (0, r)),
            pl.BlockSpec((1, half), lambda r: (0, r)),
        ),
        cost_estimate=pl.CostEstimate(
            flops=hold * 4 * frames * order * width,
            bytes_accessed=hold * frames * width * 4,
            transcendentals=0,
        ),
        name="compound",
    )(frame_count, clutter_rank, noise_rank, window, echoes, echoes, basis)


def border_kernel(window_ref, border_ref, region_ref, strength_ref, volume_ref, all_ref, sums_ref):
    frames, half = region_ref.shape
    order = border_ref.shape[0]
    lengths = strength_ref.shape[1]
    flipped = border_ref[:, half:].astype(jnp.float32).T.astype(jnp.bfloat16)[:frames, :]
    cleaned = jnp.dot(flipped, border_ref[:, :half], preferred_element_type=jnp.float32)
    cleaned = cleaned.astype(jnp.bfloat16).astype(jnp.float32)
    both = region_ref[...] + cleaned * window_ref[:, :half]
    volume_ref[...] = both
    last = jnp.sum(both * both, axis=0, keepdims=True) / frames
    all_ref[:, : lengths - half] = strength_ref[:, : lengths - half]
    all_ref[:, lengths - half :] = last
    total = jnp.sum(strength_ref[:, : lengths - half]) + jnp.sum(last)
    sums_ref[...] = jnp.full(sums_ref.shape, total, jnp.float32)


def close_border(window, border, volume, strength, hold, devices):
    frames, voxels = volume.shape
    half = voxels // hold
    return pl.pallas_call(
        border_kernel,
        grid=(1,),
        out_shape=(
            jax.ShapeDtypeStruct(volume.shape, jnp.float32),
            jax.ShapeDtypeStruct(strength.shape, jnp.float32),
            jax.ShapeDtypeStruct((devices, LANES), jnp.float32),
        ),
        in_specs=[
            pl.BlockSpec(window.shape, lambda i: (0, 0)),
            pl.BlockSpec(border.shape, lambda i: (0, 0)),
            pl.BlockSpec((frames, half), lambda i: (0, hold - 1)),
            pl.BlockSpec(strength.shape, lambda i: (0, 0)),
        ],
        out_specs=(
            pl.BlockSpec((frames, half), lambda i: (0, hold - 1)),
            pl.BlockSpec(strength.shape, lambda i: (0, 0)),
            pl.BlockSpec((devices, LANES), lambda i: (0, 0)),
        ),
        input_output_aliases={2: 0},
        name="close_border",
    )(window, border, volume, strength)


def power_kernel(strength_ref, sums_ref, power_ref):
    voxels = strength_ref.shape[1] * sums_ref.shape[0]
    total = jnp.sum(sums_ref[:, :1])
    power_ref[...] = (strength_ref[...] / (total / voxels + 1e-06))[0]


def relative_power(strength, sums):
    vmem = pl.BlockSpec(memory_space=pltpu.VMEM)
    return pl.pallas_call(
        power_kernel,
        out_shape=jax.ShapeDtypeStruct((strength.shape[1],), jnp.float32),
        in_specs=[vmem, vmem],
        out_specs=vmem,
        name="relative_power",
    )(strength, sums)


def shards(echoes, frame_count, clutter_rank, noise_rank, start_basis):
    axes = ("space", "grp")
    devices = lax.axis_size("space") * lax.axis_size("grp")
    hold, frames, width = echoes.shape
    order = start_basis.shape[1]
    window = jnp.sin(jnp.pi * (jnp.arange(width, dtype=jnp.float32) + 0.5) / width) ** 2
    window = window[None, :]
    basis, border = find_bases(echoes, frame_count, clutter_rank, noise_rank, start_basis)
    border = lax.ppermute(border, axes, [(source, source - 1) for source in range(1, devices)])
    volume, strength = compound(
        echoes, basis, window, frame_count, clutter_rank, noise_rank, order
    )
    volume, strength, sums = close_border(window, border, volume, strength, hold, devices)
    sums = lax.all_to_all(sums, axes, 0, 0, tiled=True)
    return volume, relative_power(strength, sums)


def solution(mesh):
    return jax.shard_map(
        shards,
        mesh=mesh,
        in_specs=(P(("space", "grp"), None, None), P(), P(), P(), P()),
        out_specs=(P(None, ("space", "grp")), P(("space", "grp"))),
        check_vma=False,
    )
```

```python
import jax
import jax.numpy as jnp
import numpy as np
from jax import lax
from jax.experimental import pallas as pl
from jax.experimental.pallas import tpu as pltpu
from jax.sharding import PartitionSpec as P

ITERS = 4
LANES = 128
SLOTS = 8
PANEL = 12
SUPER = 24
CHUNK = 512
SIDE = 256
VMEM_LIMIT = 24 << 20
WIDE_LIMIT = 58 << 20


def round_up(value, unit):
    return -(-value // unit) * unit


def device_index():
    return lax.axis_index("space") * lax.axis_size("grp") + lax.axis_index("grp")


def two_parts(value):
    high = value.astype(jnp.bfloat16)
    return high, (value - high.astype(jnp.float32)).astype(jnp.bfloat16)


def three_parts(value):
    high = value.astype(jnp.bfloat16)
    rest = value - high.astype(jnp.float32)
    middle = rest.astype(jnp.bfloat16)
    return high, middle, (rest - middle.astype(jnp.float32)).astype(jnp.bfloat16)


def matmul(left, right, left_axis=1, right_axis=0):
    return lax.dot_general(
        left,
        right,
        (((left_axis,), (right_axis,)), ((), ())),
        preferred_element_type=jnp.float32,
    )


def inverse_factors(rows_ref, scaled_ref, out_ref, order, hold, out_stride):
    lane = lax.broadcasted_iota(jnp.int32, (SLOTS, LANES), 1)

    def spread(value, index):
        return jnp.broadcast_to(value[:, index : index + 1], (SLOTS, LANES))

    for start in range(0, order, SUPER):
        stop = min(start + SUPER, order)
        for base in range(start, stop, PANEL):
            panel = (lane >= base) & (lane < base + PANEL)
            rows = [rows_ref[(base + r) * SLOTS : (base + r + 1) * SLOTS, :] for r in range(PANEL)]
            block = {
                (r, c): spread(rows[r], base + c) for c in range(PANEL) for r in range(c + 1)
            }
            rows = [
                jnp.where(panel, jnp.where(lane == base + r, 1.0, 0.0), rows[r])
                for r in range(PANEL)
            ]
            scaled = []
            for j in range(PANEL):
                inverse = 1.0 / block[j, j]
                scaled.append(rows[j] * inverse)
                for r in range(j + 1, PANEL):
                    factor = block[j, r] * inverse
                    rows[r] = rows[r] - factor * rows[j]
                    for c in range(r, PANEL):
                        block[r, c] = block[r, c] - factor * block[j, c]
            for j in range(PANEL):
                out_ref[pl.ds(base + j, SLOTS, stride=out_stride), :] = jnp.where(
                    lane < base + PANEL, rows[j] * lax.rsqrt(block[j, j]), 0.0
                )
            if stop < order:
                later = (lane >= base + PANEL) & (lane < stop)
                for j in range(PANEL):
                    rows_ref[(base + j) * SLOTS : (base + j + 1) * SLOTS, :] = jnp.where(
                        later, 0.0, rows[j]
                    )
                    at = base - start + j
                    scaled_ref[at * SLOTS : (at + 1) * SLOTS, :] = scaled[j]
            for r in range(base + PANEL, stop):
                total = jnp.where(panel, 0.0, rows_ref[r * SLOTS : (r + 1) * SLOTS, :])
                for j in range(PANEL):
                    total = total - spread(scaled[j], r) * rows[j]
                rows_ref[r * SLOTS : (r + 1) * SLOTS, :] = total
        if stop < order:
            rest = order - stop
            wide_lane = lax.broadcasted_iota(jnp.int32, (rest, LANES), 1)
            done = (wide_lane >= start) & (wide_lane < stop)
            for b in range(hold):
                upper = rows_ref[pl.ds(start * SLOTS + b, stop - start, stride=SLOTS), :]
                lower = scaled_ref[pl.ds(b, stop - start, stride=SLOTS), :]
                u1, u2, u3 = three_parts(upper)
                l1, l2, l3 = three_parts(lower)
                update = matmul(
                    jnp.concatenate([l1, l1, l1, l2, l2, l3], axis=0),
                    jnp.concatenate([u1, u2, u3, u1, u2, u1], axis=0),
                    0,
                    0,
                )[stop:order, :]
                where = pl.ds(stop * SLOTS + b, rest, stride=SLOTS)
                rows_ref[where, :] = jnp.where(done, 0.0, rows_ref[where, :]) - update


def basis_kernel(
    frame_hbm,
    clutter_hbm,
    noise_hbm,
    start_hbm,
    window_hbm,
    echo_hbm,
    basis_ref,
    kept_ref,
    border_ref,
    frame_ref,
    clutter_ref,
    noise_ref,
    start_ref,
    window_ref,
    small_sems,
    echo_ref,
    sems,
    gram_ref,
    sub_ref,
    prod_ref,
    rows_ref,
    scaled_ref,
    factor_ref,
):
    hold, frames, width = echo_hbm.shape
    order = start_ref.shape[0]
    tall = basis_ref.shape[1]
    deep = sub_ref.shape[1]
    half = width // 2
    first = device_index() * hold
    pairs = (
        (start_hbm, start_ref),
        (frame_hbm, frame_ref),
        (clutter_hbm, clutter_ref),
        (noise_hbm, noise_ref),
        (window_hbm, window_ref),
    )
    small = [
        pltpu.make_async_copy(source, target, small_sems.at[number])
        for number, (source, target) in enumerate(pairs)
    ]
    copies = [
        pltpu.make_async_copy(echo_hbm.at[b], echo_ref.at[b], sems.at[b]) for b in range(hold)
    ]
    for copy in (copies[0], *small, *copies[1:]):
        copy.start()
    sub_ref[...] = jnp.zeros_like(sub_ref)
    prod_ref[...] = jnp.zeros_like(prod_ref)
    rows_ref[...] = jnp.zeros_like(rows_ref)
    factor_ref[...] = jnp.zeros_like(factor_ref)
    gram_ref[...] = jnp.zeros_like(gram_ref)
    for copy in small:
        copy.wait()
    high, low = two_parts(start_ref[...].T)
    for b in range(hold):
        sub_ref[b, :frames, :order] = high
        sub_ref[b, :frames, LANES : LANES + order] = low
    row_at = lax.broadcasted_iota(jnp.int32, (frames, frames), 0)
    column_at = lax.broadcasted_iota(jnp.int32, (frames, frames), 1)
    for b in range(hold):
        copies[b].wait()
        echo = echo_ref[b]
        valid = frame_ref[first + b]
        gram = matmul(echo, echo, 1, 1)
        padding = jnp.where((row_at == column_at) & (row_at >= valid), 1.0, 0.0)
        gram = jnp.where((row_at < valid) & (column_at < valid), gram, padding)
        high, low = two_parts(gram)
        gram_ref[b, :frames, :frames] = high
        gram_ref[b, tall : tall + frames, :frames] = low

    def iteration(_, carry):
        for b in range(hold):
            terms = matmul(gram_ref[b], sub_ref[b])
            terms = terms[:tall, :] + terms[tall:, :]
            high, low = two_parts(terms[:, :LANES] + terms[:, LANES:])
            prod_ref[b, :tall, :LANES] = high
            prod_ref[b, :tall, LANES:] = low
        for b in range(hold):
            whole = prod_ref[b]
            terms = matmul(whole, whole, 0, 0)
            terms = terms[:order, :] + terms[LANES : LANES + order, :]
            rows_ref[pl.ds(b, order, stride=SLOTS), :] = terms[:, :LANES] + terms[:, LANES:]
        inverse_factors(rows_ref, scaled_ref, factor_ref, order, hold, LANES)
        for b in range(hold):
            high, low = two_parts(factor_ref[b * LANES : (b + 1) * LANES, :])
            right = jnp.concatenate(
                [
                    jnp.concatenate([high, high], axis=1),
                    jnp.concatenate([low, low], axis=1),
                ],
                axis=0,
            )
            terms = matmul(prod_ref[b, :tall, :], right, 1, 1)
            high, low = two_parts(terms[:, :LANES] + terms[:, LANES:])
            sub_ref[b, :tall, :LANES] = high
            sub_ref[b, :tall, LANES:] = low
        return carry

    lax.fori_loop(0, ITERS, iteration, 0)
    frame_at = lax.broadcasted_iota(jnp.int32, (order, deep), 1)
    column_at = lax.broadcasted_iota(jnp.int32, (order, deep), 0)
    for b in range(hold):
        basis_ref[b] = sub_ref[b, :tall, :LANES]
        flipped = sub_ref[b, :, :LANES].T[:order, :]
        at = first + b
        band = (column_at >= clutter_ref[at]) & (column_at < noise_ref[at])
        kept_ref[b] = jnp.where(
            band & (frame_at < frame_ref[at]), flipped, jnp.zeros((), jnp.bfloat16)
        )
    pieces = half // SIDE
    for piece in range(pieces):
        at = slice(piece * SIDE, (piece + 1) * SIDE)
        part = matmul(kept_ref[0, :, :frames], echo_ref[0, :, at]) * window_ref[:, at]
        border_ref[piece * order : (piece + 1) * order, :] = part.astype(jnp.bfloat16)
    start = pieces * order
    high_rows = border_ref.shape[0] - start
    border_ref[start:, :LANES] = sub_ref[0, :high_rows, :LANES]
    border_ref[start:, LANES:] = sub_ref[0, high_rows : 2 * high_rows, :LANES]


def find_bases(echoes, window, frame_count, clutter_rank, noise_rank, start_basis):
    hold, frames, width = echoes.shape
    order = start_basis.shape[1]
    tall = round_up(frames, 16)
    deep = round_up(frames, LANES)
    outside = pl.BlockSpec(memory_space=pltpu.HBM)
    vmem = pl.BlockSpec(memory_space=pltpu.VMEM)
    return pl.pallas_call(
        basis_kernel,
        out_shape=(
            jax.ShapeDtypeStruct((hold, tall, LANES), jnp.bfloat16),
            jax.ShapeDtypeStruct((hold, order, deep), jnp.bfloat16),
            jax.ShapeDtypeStruct(
                (width // 2 // SIDE * order + round_up(tall // 2, 16), SIDE), jnp.bfloat16
            ),
        ),
        in_specs=[outside] * 6,
        out_specs=(vmem, vmem, vmem),
        scratch_shapes=[
            pltpu.SMEM(frame_count.shape, jnp.int32),
            pltpu.SMEM(clutter_rank.shape, jnp.int32),
            pltpu.SMEM(noise_rank.shape, jnp.int32),
            pltpu.VMEM((order, frames), jnp.float32),
            pltpu.VMEM(window.shape, jnp.float32),
            pltpu.SemaphoreType.DMA((5,)),
            pltpu.VMEM((hold, frames, width), jnp.bfloat16),
            pltpu.SemaphoreType.DMA((hold,)),
            pltpu.VMEM((hold, 2 * tall, deep), jnp.bfloat16),
            pltpu.VMEM((hold, deep, 2 * LANES), jnp.bfloat16),
            pltpu.VMEM((hold, deep, 2 * LANES), jnp.bfloat16),
            pltpu.VMEM((order * SLOTS, LANES), jnp.float32),
            pltpu.VMEM((SUPER * SLOTS, LANES), jnp.float32),
            pltpu.VMEM((SLOTS * LANES, LANES), jnp.float32),
        ],
        name="find_bases",
    )(frame_count, clutter_rank, noise_rank, start_basis.T, window, echoes)


def region_kernel(
    window_ref,
    kept_ref,
    basis_ref,
    echo_hbm,
    volume_hbm,
    strength_ref,
    last_ref,
    echo_ref,
    coef_ref,
    volume_ref,
    load_sems,
    store_sems,
):
    hold, frames, width = echo_hbm.shape
    order = kept_ref.shape[1]
    half = width // 2
    pieces = half // CHUNK
    sides = ((1, 0), (0, 1))
    loads = {}
    for region in range(hold):
        for side, shift in sides:
            block = region + shift
            if block < hold:
                at = slice(side * half, (side + 1) * half)
                loads[region, side] = pltpu.make_async_copy(
                    echo_hbm.at[block, :, at],
                    echo_ref.at[block, :, at],
                    load_sems.at[2 * region + side],
                )
    for load in loads.values():
        load.start()
    coef_ref[...] = jnp.zeros_like(coef_ref)
    stores = []
    for step in range(hold + 1):
        for side, shift in sides:
            block = step + shift
            if step == hold or block == hold:
                continue
            loads[step, side].wait()
            for left in range(0, half, CHUNK):
                at = slice(left, left + CHUNK)
                whole = slice(side * half + left, side * half + left + CHUNK)
                part = matmul(kept_ref[block, :, :frames], echo_ref[block, :, whole])
                part = (part * window_ref[:, whole]).astype(jnp.bfloat16)
                if step == hold - 1:
                    last_ref[:, at] = part
                else:
                    top = (1 - side) * LANES
                    coef_ref[step, top : top + order, at] = part
        region = step - 1
        if region < 0 or region == hold - 1:
            continue
        pair = jnp.concatenate([basis_ref[region, :frames], basis_ref[region + 1, :frames]], axis=1)
        for piece in range(pieces):
            at = slice(piece * CHUNK, (piece + 1) * CHUNK)
            both = matmul(pair, coef_ref[region, :, at])
            where = slice(region * half + piece * CHUNK, region * half + (piece + 1) * CHUNK)
            volume_ref[:, where] = both
            strength_ref[:, where] = jnp.sum(both * both, axis=0, keepdims=True) / frames
            store = pltpu.make_async_copy(
                volume_ref.at[:, where],
                volume_hbm.at[:, where],
                store_sems.at[region * pieces + piece],
            )
            store.start()
            stores.append(store)
    for store in stores:
        store.wait()


def compound(echoes, kept, basis, window):
    hold, frames, width = echoes.shape
    order = kept.shape[1]
    half = width // 2
    inside = (hold - 1) * half
    vmem = pl.BlockSpec(memory_space=pltpu.VMEM)
    outside = pl.BlockSpec(memory_space=pltpu.HBM)
    return pl.pallas_call(
        region_kernel,
        out_shape=(
            jax.ShapeDtypeStruct((frames, hold * half), jnp.float32),
            jax.ShapeDtypeStruct((1, inside), jnp.float32),
            jax.ShapeDtypeStruct((order, half), jnp.bfloat16),
        ),
        in_specs=[vmem, vmem, vmem, outside],
        out_specs=(outside, vmem, vmem),
        scratch_shapes=[
            pltpu.VMEM((hold, frames, width), jnp.bfloat16),
            pltpu.VMEM((hold - 1, 2 * LANES, half), jnp.bfloat16),
            pltpu.VMEM((frames, inside), jnp.float32),
            pltpu.SemaphoreType.DMA((2 * hold,)),
            pltpu.SemaphoreType.DMA((inside // CHUNK,)),
        ],
        cost_estimate=pl.CostEstimate(
            flops=hold * 4 * frames * order * width,
            bytes_accessed=hold * frames * width * 4,
            transcendentals=0,
        ),
        compiler_params=pltpu.CompilerParams(vmem_limit_bytes=WIDE_LIMIT),
        name="compound",
    )(window, kept, basis, echoes)


def border_kernel(
    strength_hbm,
    own_hbm,
    basis_hbm,
    border_hbm,
    volume_in,
    volume_hbm,
    all_hbm,
    sums_ref,
    strength_ref,
    coef_ref,
    basis_ref,
    border_ref,
    volume_ref,
    load_sems,
    store_sems,
):
    frames, half = volume_ref.shape
    order = own_hbm.shape[0]
    hold = basis_hbm.shape[0]
    inside = strength_hbm.shape[1]
    pairs = (
        (border_hbm, border_ref),
        (own_hbm, coef_ref.at[:order]),
        (basis_hbm.at[hold - 1], basis_ref),
        (strength_hbm, strength_ref.at[:, :inside]),
    )
    loads = [
        pltpu.make_async_copy(source, target, load_sems.at[number])
        for number, (source, target) in enumerate(pairs)
    ]
    for load in loads:
        load.start()
    for top in (order, LANES + order):
        coef_ref[top : top + LANES - order, :] = jnp.zeros((LANES - order, half), jnp.bfloat16)
    for load in loads:
        load.wait()
    total = jnp.sum(strength_ref[:, :inside], axis=1, keepdims=True)
    start = half // SIDE * order
    following = jnp.concatenate([border_ref[start:, :LANES], border_ref[start:, LANES:]], axis=0)
    pair = jnp.concatenate([basis_ref[:frames], following[:frames]], axis=1)
    stores = []
    for number, left in enumerate(range(0, half, SIDE)):
        at = slice(left, left + SIDE)
        where = slice(inside + left, inside + left + SIDE)
        coef_ref[LANES : LANES + order, at] = border_ref[number * order : (number + 1) * order, :]
        both = matmul(pair, coef_ref[:, at])
        volume_ref[:, at] = both
        last = jnp.sum(both * both, axis=0, keepdims=True) / frames
        strength_ref[:, where] = last
        total = total + jnp.sum(last, axis=1, keepdims=True)
        store = pltpu.make_async_copy(
            volume_ref.at[:, at], volume_hbm.at[:, where], store_sems.at[number]
        )
        store.start()
        stores.append(store)
    store = pltpu.make_async_copy(strength_ref, all_hbm, store_sems.at[len(stores)])
    store.start()
    stores.append(store)
    sums_ref[...] = jnp.broadcast_to(total, sums_ref.shape)
    for store in stores:
        store.wait()


def close_border(own, basis, border, volume, strength, devices):
    order, half = own.shape
    frames, voxels = volume.shape
    tall = basis.shape[1]
    outside = pl.BlockSpec(memory_space=pltpu.HBM)
    anywhere = pl.BlockSpec(memory_space=pl.ANY)
    return pl.pallas_call(
        border_kernel,
        out_shape=(
            jax.ShapeDtypeStruct(volume.shape, jnp.float32),
            jax.ShapeDtypeStruct((1, voxels), jnp.float32),
            jax.ShapeDtypeStruct((devices, LANES), jnp.float32),
        ),
        in_specs=[anywhere] * 4 + [outside],
        out_specs=(outside, anywhere, pl.BlockSpec(memory_space=pltpu.VMEM)),
        scratch_shapes=[
            pltpu.VMEM((1, voxels), jnp.float32),
            pltpu.VMEM((2 * LANES, half), jnp.bfloat16),
            pltpu.VMEM((tall, LANES), jnp.bfloat16),
            pltpu.VMEM(border.shape, jnp.bfloat16),
            pltpu.VMEM((frames, half), jnp.float32),
            pltpu.SemaphoreType.DMA((4,)),
            pltpu.SemaphoreType.DMA((1 + half // SIDE,)),
        ],
        input_output_aliases={4: 0},
        compiler_params=pltpu.CompilerParams(vmem_limit_bytes=VMEM_LIMIT),
        name="close_border",
    )(strength, own, basis, border, volume)


def power_kernel(strength_ref, sums_ref, power_ref):
    voxels = strength_ref.shape[1] * sums_ref.shape[0]
    total = jnp.sum(sums_ref[:, :1])
    power_ref[...] = (strength_ref[...] / (total / voxels + 1e-06))[0]


def relative_power(strength, sums):
    vmem = pl.BlockSpec(memory_space=pltpu.VMEM)
    return pl.pallas_call(
        power_kernel,
        out_shape=jax.ShapeDtypeStruct((strength.shape[1],), jnp.float32),
        in_specs=[vmem, vmem],
        out_specs=vmem,
        compiler_params=pltpu.CompilerParams(vmem_limit_bytes=VMEM_LIMIT),
        name="relative_power",
    )(strength, sums)


def shards(echoes, frame_count, clutter_rank, noise_rank, start_basis):
    axes = ("space", "grp")
    devices = lax.axis_size("space") * lax.axis_size("grp")
    hold, frames, width = echoes.shape
    window = np.sin(np.pi * (np.arange(width) + 0.5) / width) ** 2
    window = jnp.asarray(window, jnp.float32)[None, :]
    basis, kept, border = find_bases(
        echoes, window, frame_count, clutter_rank, noise_rank, start_basis
    )
    border = lax.ppermute(border, axes, [(source, source - 1) for source in range(1, devices)])
    volume, strength, own = compound(echoes, kept, basis, window)
    volume, strength, sums = close_border(own, basis, border, volume, strength, devices)
    sums = lax.all_to_all(sums, axes, 0, 0, tiled=True)
    return volume, relative_power(strength, sums)


def solution(mesh):
    return jax.shard_map(
        shards,
        mesh=mesh,
        in_specs=(P(("space", "grp"), None, None), P(), P(), P(), P()),
        out_specs=(P(None, ("space", "grp")), P(("space", "grp"))),
        check_vma=False,
    )
```

```python
import jax
import jax.numpy as jnp
import numpy as np
from jax import lax
from jax.experimental import pallas as pl
from jax.experimental.pallas import tpu as pltpu
from jax.sharding import PartitionSpec as P

ITERS = 4
LANES = 128
SLOTS = 8
PANEL = 12
SUPER = 24
CHUNK = 512
SIDE = 256
VMEM_LIMIT = 24 << 20
WIDE_LIMIT = 50 << 20


def round_up(value, unit):
    return -(-value // unit) * unit


def device_index():
    return lax.axis_index("space") * lax.axis_size("grp") + lax.axis_index("grp")


def two_parts(value):
    high = value.astype(jnp.bfloat16)
    return high, (value - high.astype(jnp.float32)).astype(jnp.bfloat16)


def three_parts(value):
    high = value.astype(jnp.bfloat16)
    rest = value - high.astype(jnp.float32)
    middle = rest.astype(jnp.bfloat16)
    return high, middle, (rest - middle.astype(jnp.float32)).astype(jnp.bfloat16)


def matmul(left, right, left_axis=1, right_axis=0):
    return lax.dot_general(
        left,
        right,
        (((left_axis,), (right_axis,)), ((), ())),
        preferred_element_type=jnp.float32,
    )


def inverse_factors(rows_ref, scaled_ref, out_ref, order, hold, out_stride):
    lane = lax.broadcasted_iota(jnp.int32, (SLOTS, LANES), 1)

    def spread(value, index):
        return jnp.broadcast_to(value[:, index : index + 1], (SLOTS, LANES))

    for start in range(0, order, SUPER):
        stop = min(start + SUPER, order)
        for base in range(start, stop, PANEL):
            panel = (lane >= base) & (lane < base + PANEL)
            rows = [rows_ref[(base + r) * SLOTS : (base + r + 1) * SLOTS, :] for r in range(PANEL)]
            block = {
                (r, c): spread(rows[r], base + c) for c in range(PANEL) for r in range(c + 1)
            }
            rows = [
                jnp.where(panel, jnp.where(lane == base + r, 1.0, 0.0), rows[r])
                for r in range(PANEL)
            ]
            scaled = []
            for j in range(PANEL):
                inverse = 1.0 / block[j, j]
                scaled.append(rows[j] * inverse)
                for r in range(j + 1, PANEL):
                    factor = block[j, r] * inverse
                    rows[r] = rows[r] - factor * rows[j]
                    for c in range(r, PANEL):
                        block[r, c] = block[r, c] - factor * block[j, c]
            for j in range(PANEL):
                out_ref[pl.ds(base + j, SLOTS, stride=out_stride), :] = jnp.where(
                    lane < base + PANEL, rows[j] * lax.rsqrt(block[j, j]), 0.0
                )
            if stop < order:
                later = (lane >= base + PANEL) & (lane < stop)
                for j in range(PANEL):
                    rows_ref[(base + j) * SLOTS : (base + j + 1) * SLOTS, :] = jnp.where(
                        later, 0.0, rows[j]
                    )
                    at = base - start + j
                    scaled_ref[at * SLOTS : (at + 1) * SLOTS, :] = scaled[j]
            for r in range(base + PANEL, stop):
                total = jnp.where(panel, 0.0, rows_ref[r * SLOTS : (r + 1) * SLOTS, :])
                for j in range(PANEL):
                    total = total - spread(scaled[j], r) * rows[j]
                rows_ref[r * SLOTS : (r + 1) * SLOTS, :] = total
        if stop < order:
            rest = order - stop
            wide_lane = lax.broadcasted_iota(jnp.int32, (rest, LANES), 1)
            done = (wide_lane >= start) & (wide_lane < stop)
            for b in range(hold):
                upper = rows_ref[pl.ds(start * SLOTS + b, stop - start, stride=SLOTS), :]
                lower = scaled_ref[pl.ds(b, stop - start, stride=SLOTS), :]
                u1, u2, u3 = three_parts(upper)
                l1, l2, l3 = three_parts(lower)
                update = matmul(
                    jnp.concatenate([l1, l1, l1, l2, l2, l3], axis=0),
                    jnp.concatenate([u1, u2, u3, u1, u2, u1], axis=0),
                    0,
                    0,
                )[stop:order, :]
                where = pl.ds(stop * SLOTS + b, rest, stride=SLOTS)
                rows_ref[where, :] = jnp.where(done, 0.0, rows_ref[where, :]) - update


def basis_kernel(
    frame_hbm,
    clutter_hbm,
    noise_hbm,
    start_hbm,
    window_hbm,
    echo_hbm,
    basis_ref,
    kept_ref,
    border_ref,
    frame_ref,
    clutter_ref,
    noise_ref,
    start_ref,
    window_ref,
    small_sems,
    echo_ref,
    sems,
    gram_ref,
    sub_ref,
    prod_ref,
    rows_ref,
    scaled_ref,
    factor_ref,
):
    hold, frames, width = echo_hbm.shape
    order = start_ref.shape[0]
    tall = basis_ref.shape[1]
    deep = sub_ref.shape[1]
    half = width // 2
    first = device_index() * hold
    pairs = (
        (start_hbm, start_ref),
        (frame_hbm, frame_ref),
        (clutter_hbm, clutter_ref),
        (noise_hbm, noise_ref),
        (window_hbm, window_ref),
    )
    small = [
        pltpu.make_async_copy(source, target, small_sems.at[number])
        for number, (source, target) in enumerate(pairs)
    ]
    copies = [
        pltpu.make_async_copy(echo_hbm.at[b], echo_ref.at[b], sems.at[b]) for b in range(hold)
    ]
    for copy in (copies[0], *small, *copies[1:]):
        copy.start()
    sub_ref[...] = jnp.zeros_like(sub_ref)
    prod_ref[...] = jnp.zeros_like(prod_ref)
    rows_ref[...] = jnp.zeros_like(rows_ref)
    factor_ref[...] = jnp.zeros_like(factor_ref)
    gram_ref[...] = jnp.zeros_like(gram_ref)
    for copy in small:
        copy.wait()
    high, low = two_parts(start_ref[...].T)
    for b in range(hold):
        sub_ref[b, :frames, :order] = high
        sub_ref[b, :frames, LANES : LANES + order] = low
    row_at = lax.broadcasted_iota(jnp.int32, (frames, frames), 0)
    column_at = lax.broadcasted_iota(jnp.int32, (frames, frames), 1)
    for b in range(hold):
        copies[b].wait()
        echo = echo_ref[b]
        valid = frame_ref[first + b]
        gram = matmul(echo, echo, 1, 1)
        padding = jnp.where((row_at == column_at) & (row_at >= valid), 1.0, 0.0)
        gram = jnp.where((row_at < valid) & (column_at < valid), gram, padding)
        high, low = two_parts(gram)
        gram_ref[b, :frames, :frames] = high
        gram_ref[b, tall : tall + frames, :frames] = low

    def iteration(_, carry):
        for b in range(hold):
            terms = matmul(gram_ref[b], sub_ref[b])
            terms = terms[:tall, :] + terms[tall:, :]
            high, low = two_parts(terms[:, :LANES] + terms[:, LANES:])
            prod_ref[b, :tall, :LANES] = high
            prod_ref[b, :tall, LANES:] = low
        for b in range(hold):
            whole = prod_ref[b]
            terms = matmul(whole, whole, 0, 0)
            terms = terms[:order, :] + terms[LANES : LANES + order, :]
            rows_ref[pl.ds(b, order, stride=SLOTS), :] = terms[:, :LANES] + terms[:, LANES:]
        inverse_factors(rows_ref, scaled_ref, factor_ref, order, hold, LANES)
        for b in range(hold):
            high, low = two_parts(factor_ref[b * LANES : (b + 1) * LANES, :])
            right = jnp.concatenate(
                [
                    jnp.concatenate([high, high], axis=1),
                    jnp.concatenate([low, low], axis=1),
                ],
                axis=0,
            )
            terms = matmul(prod_ref[b, :tall, :], right, 1, 1)
            high, low = two_parts(terms[:, :LANES] + terms[:, LANES:])
            sub_ref[b, :tall, :LANES] = high
            sub_ref[b, :tall, LANES:] = low
        return carry

    lax.fori_loop(0, ITERS, iteration, 0)
    frame_at = lax.broadcasted_iota(jnp.int32, (order, deep), 1)
    column_at = lax.broadcasted_iota(jnp.int32, (order, deep), 0)
    for b in range(hold):
        basis_ref[b] = sub_ref[b, :tall, :LANES]
        flipped = sub_ref[b, :, :LANES].T[:order, :]
        at = first + b
        band = (column_at >= clutter_ref[at]) & (column_at < noise_ref[at])
        kept_ref[b] = jnp.where(
            band & (frame_at < frame_ref[at]), flipped, jnp.zeros((), jnp.bfloat16)
        )
    pieces = half // SIDE
    for piece in range(pieces):
        at = slice(piece * SIDE, (piece + 1) * SIDE)
        part = matmul(kept_ref[0, :, :frames], echo_ref[0, :, at]) * window_ref[:, at]
        border_ref[piece * order : (piece + 1) * order, :] = part.astype(jnp.bfloat16)
    start = pieces * order
    high_rows = border_ref.shape[0] - start
    border_ref[start:, :LANES] = sub_ref[0, :high_rows, :LANES]
    border_ref[start:, LANES:] = sub_ref[0, high_rows : 2 * high_rows, :LANES]


def find_bases(echoes, window, frame_count, clutter_rank, noise_rank, start_basis):
    hold, frames, width = echoes.shape
    order = start_basis.shape[1]
    tall = round_up(frames, 16)
    deep = round_up(frames, LANES)
    outside = pl.BlockSpec(memory_space=pltpu.HBM)
    vmem = pl.BlockSpec(memory_space=pltpu.VMEM)
    return pl.pallas_call(
        basis_kernel,
        out_shape=(
            jax.ShapeDtypeStruct((hold, tall, LANES), jnp.bfloat16),
            jax.ShapeDtypeStruct((hold, order, deep), jnp.bfloat16),
            jax.ShapeDtypeStruct(
                (width // 2 // SIDE * order + round_up(tall // 2, 16), SIDE), jnp.bfloat16
            ),
        ),
        in_specs=[outside] * 6,
        out_specs=(vmem, vmem, vmem),
        scratch_shapes=[
            pltpu.SMEM(frame_count.shape, jnp.int32),
            pltpu.SMEM(clutter_rank.shape, jnp.int32),
            pltpu.SMEM(noise_rank.shape, jnp.int32),
            pltpu.VMEM((order, frames), jnp.float32),
            pltpu.VMEM(window.shape, jnp.float32),
            pltpu.SemaphoreType.DMA((5,)),
            pltpu.VMEM((hold, frames, width), jnp.bfloat16),
            pltpu.SemaphoreType.DMA((hold,)),
            pltpu.VMEM((hold, 2 * tall, deep), jnp.bfloat16),
            pltpu.VMEM((hold, deep, 2 * LANES), jnp.bfloat16),
            pltpu.VMEM((hold, deep, 2 * LANES), jnp.bfloat16),
            pltpu.VMEM((order * SLOTS, LANES), jnp.float32),
            pltpu.VMEM((SUPER * SLOTS, LANES), jnp.float32),
            pltpu.VMEM((SLOTS * LANES, LANES), jnp.float32),
        ],
        name="find_bases",
    )(frame_count, clutter_rank, noise_rank, start_basis.T, window, echoes)


def region_kernel(
    window_ref,
    kept_ref,
    basis_ref,
    echo_hbm,
    volume_hbm,
    strength_ref,
    last_ref,
    echo_ref,
    coef_ref,
    volume_ref,
    load_sems,
    store_sems,
):
    hold, frames, width = echo_hbm.shape
    order = kept_ref.shape[1]
    half = width // 2
    pieces = half // CHUNK
    sides = ((1, 0), (0, 1))
    loads = {}
    for region in range(hold):
        for side, shift in sides:
            block = region + shift
            if block < hold:
                at = slice(side * half, (side + 1) * half)
                loads[region, side] = pltpu.make_async_copy(
                    echo_hbm.at[block, :, at],
                    echo_ref.at[block, :, at],
                    load_sems.at[2 * region + side],
                )
    for load in loads.values():
        load.start()
    coef_ref[...] = jnp.zeros_like(coef_ref)
    stores = []
    for step in range(hold + 1):
        for side, shift in sides:
            block = step + shift
            if step == hold or block == hold:
                continue
            loads[step, side].wait()
            for left in range(0, half, CHUNK):
                at = slice(left, left + CHUNK)
                whole = slice(side * half + left, side * half + left + CHUNK)
                part = matmul(kept_ref[block, :, :frames], echo_ref[block, :, whole])
                part = (part * window_ref[:, whole]).astype(jnp.bfloat16)
                if step == hold - 1:
                    last_ref[:, at] = part
                else:
                    top = (1 - side) * LANES
                    coef_ref[step, top : top + order, at] = part
        region = step - 1
        if region < 0 or region == hold - 1:
            continue
        pair = jnp.concatenate([basis_ref[region, :frames], basis_ref[region + 1, :frames]], axis=1)
        for piece in range(pieces):
            at = slice(piece * CHUNK, (piece + 1) * CHUNK)
            both = matmul(pair, coef_ref[region, :, at])
            where = slice(region * half + piece * CHUNK, region * half + (piece + 1) * CHUNK)
            volume_ref[:, where] = both
            strength_ref[:, where] = jnp.sum(both * both, axis=0, keepdims=True) / frames
            store = pltpu.make_async_copy(
                volume_ref.at[:, where],
                volume_hbm.at[:, where],
                store_sems.at[region * pieces + piece],
            )
            store.start()
            stores.append(store)
    for store in stores:
        store.wait()


def compound(echoes, kept, basis, window):
    hold, frames, width = echoes.shape
    order = kept.shape[1]
    half = width // 2
    inside = (hold - 1) * half
    vmem = pl.BlockSpec(memory_space=pltpu.VMEM)
    outside = pl.BlockSpec(memory_space=pltpu.HBM)
    return pl.pallas_call(
        region_kernel,
        out_shape=(
            jax.ShapeDtypeStruct((frames, hold * half), jnp.float32),
            jax.ShapeDtypeStruct((1, inside), jnp.float32),
            jax.ShapeDtypeStruct((order, half), jnp.bfloat16),
        ),
        in_specs=[vmem, vmem, vmem, outside],
        out_specs=(outside, vmem, vmem),
        scratch_shapes=[
            pltpu.VMEM((hold, frames, width), jnp.bfloat16),
            pltpu.VMEM((hold - 1, 2 * LANES, half), jnp.bfloat16),
            pltpu.VMEM((frames, inside), jnp.float32),
            pltpu.SemaphoreType.DMA((2 * hold,)),
            pltpu.SemaphoreType.DMA((inside // CHUNK,)),
        ],
        cost_estimate=pl.CostEstimate(
            flops=hold * 4 * frames * order * width,
            bytes_accessed=hold * frames * width * 4,
            transcendentals=0,
        ),
        compiler_params=pltpu.CompilerParams(vmem_limit_bytes=WIDE_LIMIT),
        name="compound",
    )(window, kept, basis, echoes)


def border_kernel(
    strength_hbm,
    own_hbm,
    basis_hbm,
    border_hbm,
    volume_in,
    volume_hbm,
    all_hbm,
    sums_ref,
    strength_ref,
    coef_ref,
    basis_ref,
    border_ref,
    volume_ref,
    load_sems,
    store_sems,
):
    frames, half = volume_ref.shape
    order = own_hbm.shape[0]
    hold = basis_hbm.shape[0]
    inside = strength_hbm.shape[1]
    pairs = (
        (border_hbm, border_ref),
        (own_hbm, coef_ref.at[:order]),
        (basis_hbm.at[hold - 1], basis_ref),
        (strength_hbm, strength_ref.at[:, :inside]),
    )
    loads = [
        pltpu.make_async_copy(source, target, load_sems.at[number])
        for number, (source, target) in enumerate(pairs)
    ]
    for load in loads:
        load.start()
    for top in (order, LANES + order):
        coef_ref[top : top + LANES - order, :] = jnp.zeros((LANES - order, half), jnp.bfloat16)
    for load in loads:
        load.wait()
    total = jnp.sum(strength_ref[:, :inside], axis=1, keepdims=True)
    start = half // SIDE * order
    following = jnp.concatenate([border_ref[start:, :LANES], border_ref[start:, LANES:]], axis=0)
    pair = jnp.concatenate([basis_ref[:frames], following[:frames]], axis=1)
    stores = []
    for number, left in enumerate(range(0, half, SIDE)):
        at = slice(left, left + SIDE)
        where = slice(inside + left, inside + left + SIDE)
        coef_ref[LANES : LANES + order, at] = border_ref[number * order : (number + 1) * order, :]
        both = matmul(pair, coef_ref[:, at])
        volume_ref[:, at] = both
        last = jnp.sum(both * both, axis=0, keepdims=True) / frames
        strength_ref[:, where] = last
        total = total + jnp.sum(last, axis=1, keepdims=True)
        store = pltpu.make_async_copy(
            volume_ref.at[:, at], volume_hbm.at[:, where], store_sems.at[number]
        )
        store.start()
        stores.append(store)
    store = pltpu.make_async_copy(strength_ref, all_hbm, store_sems.at[len(stores)])
    store.start()
    stores.append(store)
    sums_ref[...] = jnp.broadcast_to(total, sums_ref.shape)
    for store in stores:
        store.wait()


def close_border(own, basis, border, volume, strength, devices):
    order, half = own.shape
    frames, voxels = volume.shape
    tall = basis.shape[1]
    outside = pl.BlockSpec(memory_space=pltpu.HBM)
    anywhere = pl.BlockSpec(memory_space=pl.ANY)
    return pl.pallas_call(
        border_kernel,
        out_shape=(
            jax.ShapeDtypeStruct(volume.shape, jnp.float32),
            jax.ShapeDtypeStruct((1, voxels), jnp.float32),
            jax.ShapeDtypeStruct((devices, LANES), jnp.float32),
        ),
        in_specs=[anywhere] * 4 + [outside],
        out_specs=(outside, anywhere, pl.BlockSpec(memory_space=pltpu.VMEM)),
        scratch_shapes=[
            pltpu.VMEM((1, voxels), jnp.float32),
            pltpu.VMEM((2 * LANES, half), jnp.bfloat16),
            pltpu.VMEM((tall, LANES), jnp.bfloat16),
            pltpu.VMEM(border.shape, jnp.bfloat16),
            pltpu.VMEM((frames, half), jnp.float32),
            pltpu.SemaphoreType.DMA((4,)),
            pltpu.SemaphoreType.DMA((1 + half // SIDE,)),
        ],
        input_output_aliases={4: 0},
        compiler_params=pltpu.CompilerParams(vmem_limit_bytes=VMEM_LIMIT),
        name="close_border",
    )(strength, own, basis, border, volume)


def power_kernel(strength_ref, sums_ref, power_ref):
    voxels = strength_ref.shape[1] * sums_ref.shape[0]
    total = jnp.sum(sums_ref[:, :1])
    power_ref[...] = (strength_ref[...] / (total / voxels + 1e-06))[0]


def relative_power(strength, sums):
    vmem = pl.BlockSpec(memory_space=pltpu.VMEM)
    return pl.pallas_call(
        power_kernel,
        out_shape=jax.ShapeDtypeStruct((strength.shape[1],), jnp.float32),
        in_specs=[vmem, vmem],
        out_specs=vmem,
        compiler_params=pltpu.CompilerParams(vmem_limit_bytes=VMEM_LIMIT),
        name="relative_power",
    )(strength, sums)


def shards(echoes, frame_count, clutter_rank, noise_rank, start_basis):
    axes = ("space", "grp")
    devices = lax.axis_size("space") * lax.axis_size("grp")
    hold, frames, width = echoes.shape
    window = np.sin(np.pi * (np.arange(width) + 0.5) / width) ** 2
    window = jnp.asarray(window, jnp.float32)[None, :]
    basis, kept, border = find_bases(
        echoes, window, frame_count, clutter_rank, noise_rank, start_basis
    )
    border = lax.ppermute(border, axes, [(source, source - 1) for source in range(1, devices)])
    volume, strength, own = compound(echoes, kept, basis, window)
    volume, strength, sums = close_border(own, basis, border, volume, strength, devices)
    sums = lax.all_to_all(sums, axes, 0, 0, tiled=True)
    return volume, relative_power(strength, sums)


def solution(mesh):
    return jax.shard_map(
        shards,
        mesh=mesh,
        in_specs=(P(("space", "grp"), None, None), P(), P(), P(), P()),
        out_specs=(P(None, ("space", "grp")), P(("space", "grp"))),
        check_vma=False,
    )
```
